256 devices in a mesh: dp: 4 (over z_hi, core), vocab: 64 (over y, z_lo, x).
Axes of the slice: x: 4, y: 4, z: 8 (z_hi: 2, z_lo: 4; z = z_hi * 4 + z_lo), core: 2. Of those that a mesh axis runs over, the one named last changes fastest.
Arguments:
- hidden: bfloat16 [2048, 4608], P(('dp', 'vocab')), may hold values from -6 to 6
- embedding: bfloat16 [32768, 4608], P('vocab'), may hold values from -0.25 to 0.25
- targets: int32 [2048], P('dp'), may hold values from 0 to 32767
- grammar_bits: int32 [2048, 1024], P('dp', 'vocab'), may hold values from -2147483648 to 2147483647, as said below
Outputs:
- token_loss: float32 [2048], P('dp')
- hidden_grad: float32 [2048, 4608], P(('dp', 'vocab'))
- embed_grad: float32 [32768, 4608], P('vocab', 'dp')
The draws below stay inside these ranges and needn't reach their ends.
Inputs may be any that keep to these rules, and one draw needn't show every extreme that they name: `grammar_bits`: bit b of word k of a token's row stands for vocabulary entry 32 k + b. Each 128-entry block of a row is either drawn at random or all zero, with a share of zero blocks that differs from block to block of the vocabulary.
All inputs are finite; a program needn't handle non-finite values.
Results may differ from the reference program's by a relative error of at most 0.0023.
Values may be sent and summed in bfloat16 or wider, within the bound.
A program may use at most 128 MiB of HBM per device.

```python
import math
import jax
import jax.numpy as jnp
import numpy as np
from jax import lax

D = 4608
VOCAB = 32768
TOKENS = 2048


def draw_grammar_bits(key, part):
    word_count = VOCAB // 32
    key_list = jax.random.split(jax.random.fold_in(key, 17), 4)
    upper_half = jax.random.randint(key_list[0], (TOKENS, word_count), 0, 65536, dtype=jnp.int32)
    lower_half = jax.random.randint(key_list[1], (TOKENS, word_count), 0, 65536, dtype=jnp.int32)
    packed = (upper_half - 32768) * 65536 + lower_half
    block_level = jax.random.randint(key_list[2], (1, VOCAB // 128), 10, 90, dtype=jnp.int32)
    block_roll = jax.random.randint(key_list[3], (TOKENS, VOCAB // 128), 0, 100, dtype=jnp.int32)
    block_keep = (block_roll < block_level).astype(jnp.int32)
    block_keep = jnp.repeat(block_keep, 4, axis=1)
    return packed * block_keep


def touch_ends(result, stream_key, smallest, top_value):
    extent = result.shape
    place = [jax.random.randint(jax.random.fold_in(stream_key, axis), (), 0, extent[axis]) for axis in range(len(extent))]
    result = result.at[tuple(place)].set(smallest)
    longest = extent.index(max(extent))
    place[longest] = (place[longest] + 1) % extent[longest]
    return result.at[tuple(place)].set(top_value)


def block_scale(rng, shape, cuts, smallest, high):
    def one(dim, shards_of):
        draws = jax.random.uniform(jax.random.fold_in(jax.random.fold_in(rng, 6), dim), (shards_of,), jnp.float32, smallest / len(cuts), high / len(cuts))
        return jnp.repeat(jnp.exp(draws), shape[dim] // shards_of).reshape((-1,) + (1,) * (len(shape) - dim - 1))

    level = one(*cuts[0])
    for cut in cuts[1:]:
        level = level * one(*cut)
    return level


def cumulative_ranks(number_of, slope):
    portions = [(1 << 20) // math.isqrt(grade ** slope) + 1 for grade in range(1, number_of + 1)]
    width = 1 + sum(portions) // (1 << 30)
    return np.cumsum(np.array([max(1, weight // width) for weight in portions]))


def skewed_ids(key, shape, number_of, slope):
    listing = cumulative_ranks(number_of, slope)
    pick = jax.random.randint(jax.random.fold_in(key, 1), shape, 0, int(listing[number_of - 1]))
    grade = jnp.searchsorted(jnp.asarray(listing, jnp.int32), pick, side="right")
    return jax.random.permutation(jax.random.fold_in(key, 2), number_of)[grade].astype(jnp.int32)


def normal_values(stream_key, shape, deviation, bound, cuts=(), kind=jnp.bfloat16):
    level = block_scale(stream_key, shape, cuts, -0.22, 0.18) if cuts else 1.0
    result = jax.random.normal(stream_key, shape, jnp.float32) * deviation * level
    return jnp.minimum(jnp.maximum(result, -bound), bound).astype(kind)


def setup_inputs(seed: int = 0) -> dict:
    splits = jax.random.split(jax.random.key(seed), 5)
    return {
        "hidden": normal_values(splits[0], (TOKENS, D), 1.0, 6.0, ((0, 256),)),
        "embedding": normal_values(splits[1], (VOCAB, D), (D // 9) ** -0.5, 0.25, ((0, 64),)),
        "targets": touch_ends(skewed_ids(splits[2], (TOKENS,), VOCAB, 2), jax.random.fold_in(splits[2], 3), 0, VOCAB - 1).astype(jnp.int32),
        "grammar_bits": draw_grammar_bits(jax.random.fold_in(splits[4], 71), 0),
    }


softcap = 30.0


def reference(hidden, embedding, targets, grammar_bits):
    row_count = hidden.shape[0]
    block_rows = math.gcd(row_count, 256)
    block_count = row_count // block_rows
    vocab_count = embedding.shape[0]
    vocab_ids = jnp.arange(vocab_count, dtype=jnp.int32)
    shifts = jnp.arange(32, dtype=jnp.int32)

    def one_block(running, inputs):
        hidden_block, target_block, bit_block = inputs
        scores = jnp.dot(hidden_block, embedding.T, preferred_element_type=jnp.float32)
        capped = softcap * jnp.tanh(scores / softcap)
        unpacked = jnp.right_shift(bit_block[:, :, None], shifts[None, None, :]) & 1
        unpacked = unpacked.reshape(block_rows, vocab_count)
        onehot = vocab_ids[None, :] == target_block[:, None]
        allowed = (unpacked == 1) | onehot
        totals = jnp.sum(jnp.where(allowed, jnp.exp(capped), 0.0), axis=1)
        log_total = jnp.log(totals)
        target_logit = jnp.sum(jnp.where(onehot, capped, 0.0), axis=1)
        block_loss = log_total - target_logit
        probability = jnp.where(allowed, jnp.exp(capped - log_total[:, None]), 0.0)
        softcap_slope = 1.0 - jnp.square(capped / softcap)
        dlogit = ((probability - onehot.astype(jnp.float32)) * softcap_slope).astype(jnp.bfloat16)
        block_hidden_grad = jnp.dot(dlogit, embedding, preferred_element_type=jnp.float32)
        running = running + jnp.dot(dlogit.T, hidden_block, preferred_element_type=jnp.float32)
        return running, (block_loss, block_hidden_grad)

    zero_grad = jnp.zeros((vocab_count, hidden.shape[1]), jnp.float32)
    embed_grad, (block_loss, block_hidden_grad) = lax.scan(
        one_block,
        zero_grad,
        (hidden.reshape(block_count, block_rows, hidden.shape[1]),
         targets.reshape(block_count, block_rows),
         grammar_bits.reshape(block_count, block_rows, grammar_bits.shape[1])))
    token_loss = block_loss.reshape(row_count)
    hidden_grad = block_hidden_grad.reshape(row_count, hidden.shape[1])
    return token_loss, hidden_grad, embed_grad
```

```python
import functools

import jax
import jax.numpy as jnp
from jax import lax
from jax.experimental import pallas as pl
from jax.experimental.pallas import tpu as pltpu
from jax.sharding import Mesh
from jax.sharding import PartitionSpec as P

AXES = ("dp_0", "dp_1", "vocab_0", "vocab_1", "vocab_2")
VOCAB = ("vocab_0", "vocab_1", "vocab_2")
DP = ("dp_0", "dp_1")
HALF, CORE, Y, Z, X = AXES
MESH = pl.DeviceIdType.MESH
N = 4
ROWS = 8
softcap = 30.0
F32, BF16 = jnp.float32, jnp.bfloat16


def fold(k):
    return lax.rem(k, N)


def masks(words, targets, first_id):
    rows = 32 * words.shape[0]
    bit = lax.broadcasted_iota(jnp.int32, (32, words.shape[1]), 0)
    spread = [jnp.right_shift(words[k : k + 1], bit) & 1 for k in range(words.shape[0])]
    unpacked = spread[0] if len(spread) == 1 else jnp.concatenate(spread, axis=0)
    ids = first_id + lax.broadcasted_iota(jnp.int32, (rows, words.shape[1]), 0)
    onehot = ids == targets
    return (unpacked == 1) | onehot, onehot


class Mail:
    def __init__(self, send_sem, recv_sem):
        self.send_sem, self.recv_sem = send_sem, recv_sem
        self.count = 0
        self.sent = []

    def post(self, src, dst, device):
        k = self.count
        self.count += 1
        copy = pltpu.make_async_remote_copy(
            src_ref=src,
            dst_ref=dst,
            send_sem=self.send_sem.at[k],
            recv_sem=self.recv_sem.at[k],
            device_id=device,
            device_id_type=MESH,
        )
        copy.start()
        self.sent.append(copy)
        return copy

    def close(self):
        for copy in self.sent:
            copy.wait_send()


class Gather:
    def __init__(self, mail, view, at, first, second):
        self.mail, self.view = mail, view
        self.first, self.second = first, second
        self.u, self.v = at[first], at[second]
        self.planes = []

    def ref(self, u, v, start=0, size=N):
        y, x = (u, v) if self.first == Y else (v, u)
        return self.view(y, pl.ds(start, size), x)

    def near(self, axis, ref):
        k = self.u if axis == self.first else self.v
        return [self.mail.post(ref, ref, {axis: fold(k + d)}) for d in (1, N - 1)]

    def along_first(self):
        self.plus, self.minus = self.near(self.first, self.ref(self.u, self.v))

    def plane(self, d):
        p = fold(self.u + d)
        self.planes.append((p, self.near(self.second, self.ref(p, self.v))))

    def relay_first(self):
        before, after = fold(self.u + N - 1), fold(self.u + 1)
        self.plus.wait_recv()
        low = self.ref(before, self.v, 0, 2)
        self.far = [self.mail.post(low, low, {self.first: after})]
        self.minus.wait_recv()
        high = self.ref(after, self.v, 2, 2)
        self.far.append(self.mail.post(high, high, {self.first: before}))
        self.relays = []

    def far_first(self):
        for copy in self.far:
            copy.wait_recv()

    def relay_second(self, k):
        before, after = fold(self.v + N - 1), fold(self.v + 1)
        p, (plus, minus) = self.planes[k]
        plus.wait_recv()
        low = self.ref(p, before, 0, 2)
        self.relays.append(self.mail.post(low, low, {self.second: after}))
        minus.wait_recv()
        high = self.ref(p, after, 2, 2)
        self.relays.append(self.mail.post(high, high, {self.second: before}))

    def finish(self):
        for copy in self.relays:
            copy.wait_recv()


class Reduce:
    def __init__(self, mail, part, boxes, at, first, second, out, columns):
        self.mail, self.part, self.at = mail, part, at
        self.send1, self.recv1, self.mid, self.send2, self.recv2, self.last, self.send3, self.recv3 = boxes
        self.first, self.second = first, second
        self.u, self.w = at[first], at[second]
        self.out, self.columns = out, columns

    def partial(self, u, w, start):
        y, x = (w, u) if self.first == X else (u, w)
        return self.part[y, pl.ds(start, 2), x]

    def post1(self, k, d):
        return self.mail.post(self.send1.at[k], self.recv1.at[k], {self.first: fold(self.u + d)})

    def post2(self, k, d):
        return self.mail.post(self.send2.at[k], self.recv2.at[k], {self.second: fold(self.w + d)})

    def open1(self):
        self.one = []
        plan = ((2, 0, 1), (2, 2, N - 1), (1, 2, 1), (N - 1, 0, N - 1))
        for k, (to, start, d) in enumerate(plan):
            u = fold(self.u + to)

            def stage(w, _):
                self.send1[k, w] = self.partial(u, w, start).astype(BF16)
                return _

            lax.fori_loop(0, N, stage, 0)
            self.one.append(self.post1(k, d))

    def relay1(self):
        for k, to, start in ((0, 1, 0), (1, N - 1, 2)):
            self.one[k].wait_recv()
            u = fold(self.u + to)

            def stage(w, _):
                total = self.partial(u, w, start) + self.recv1[k, w].astype(F32)
                self.send1[4 + k, w] = total.astype(BF16)
                return _

            lax.fori_loop(0, N, stage, 0)
            self.one.append(self.post1(4 + k, to))

    def open2(self):
        for k in (2, 3, 4, 5):
            self.one[k].wait_recv()

        def total(w, _):
            self.mid[w, 0:2] = (
                self.partial(self.u, w, 0) + self.recv1[3, w].astype(F32) + self.recv1[4, w].astype(F32)
            )
            self.mid[w, 2:4] = (
                self.partial(self.u, w, 2) + self.recv1[2, w].astype(F32) + self.recv1[5, w].astype(F32)
            )
            return _

        lax.fori_loop(0, N, total, 0)
        self.two = []
        plan = ((2, 0, 1), (2, 2, N - 1), (1, 2, 1), (N - 1, 0, N - 1))
        for k, (to, start, d) in enumerate(plan):
            self.send2[k] = self.mid[fold(self.w + to), start : start + 2].astype(self.send2.dtype)
            self.two.append(self.post2(k, d))

    def relay2(self):
        for k, to, start in ((0, 1, 0), (1, N - 1, 2)):
            self.two[k].wait_recv()
            total = self.mid[fold(self.w + to), start : start + 2] + self.recv2[k].astype(F32)
            self.send2[4 + k] = total.astype(self.send2.dtype)
            self.two.append(self.post2(4 + k, to))

    def open3(self):
        for k in (2, 3, 4, 5):
            self.two[k].wait_recv()
        self.last[0:2] = self.mid[self.w, 0:2] + self.recv2[3].astype(F32) + self.recv2[4].astype(F32)
        self.last[2:4] = self.mid[self.w, 2:4] + self.recv2[2].astype(F32) + self.recv2[5].astype(F32)
        self.three = []
        for d in range(1, N):
            z = fold(self.at[Z] + d)
            self.send3[d - 1] = self.last[z].astype(BF16)
            self.three.append(self.mail.post(self.send3.at[d - 1], self.recv3.at[d - 1], {Z: z}))

    def finish(self):
        total = self.last[self.at[Z]]
        for d in range(1, N):
            self.three[d - 1].wait_recv()
            total += self.recv3[d - 1].astype(F32)
        self.out[:, self.columns] = total


def kernel(
    hidden, words, targets, embedding_hbm,
    loss, hidden_grad, embed_grad,
    tokens, extra, sibling, embedding, scores, dlogits, by_token, part, sums,
    send1, recv1, mid, send2, recv2, last, send3, recv3,
    load_sem, send_sem, recv_sem,
):
    at = {a: lax.axis_index(a) for a in AXES}
    half, core, y, z, x = (at[a] for a in AXES)
    width = hidden.shape[1]
    vocab_local = embedding.shape[0]
    group = tokens.shape[0] * tokens.shape[1] * tokens.shape[2] * ROWS
    color, share, lane = width // 2, width // 4, width // 4
    partner = {HALF: 1 - half}
    across = {HALF: 1 - half, CORE: 1 - core}
    other = {CORE: 1 - core}
    vocab_start = ((y * N + z) * N + x) * vocab_local

    load = pltpu.make_async_copy(embedding_hbm, embedding, load_sem)
    load.start()
    barrier = pltpu.get_barrier_semaphore()
    greeted = [{a: fold(at[a] + d)} for a in (X, Y, Z) for d in range(1, N)] + [partner, across, other]
    for device in greeted:
        pl.semaphore_signal(barrier, inc=1, device_id=device, device_id_type=MESH)
    pl.semaphore_wait(barrier, len(greeted))

    mail = Mail(send_sem, recv_sem)
    own = [mail.post(hidden, tokens.at[y, z, x], {Z: fold(z + d)}) for d in (1, N - 1, 2)]

    def share_of(h, c):
        return pl.ds(pl.multiple_of((2 * h + c) * share, 128), share)

    crossed = [
        mail.post(hidden.at[:, share_of(1 - half, core)], extra.at[0, y, z, x], partner),
        mail.post(hidden.at[:, share_of(1 - half, 1 - core)], extra.at[1, y, z, x], across),
    ]
    tokens[y, z, x] = hidden[...]

    def main_view(start):
        return lambda yy, zz, xx: tokens.at[yy, zz, xx, :, pl.ds(start, color)]

    def extra_view(k):
        return lambda yy, zz, xx: extra.at[k, yy, zz, xx]

    mains = [Gather(mail, main_view(0), at, Y, X), Gather(mail, main_view(color), at, X, Y)]
    extras = [Gather(mail, extra_view(0), at, Y, X), Gather(mail, extra_view(1), at, X, Y)]

    for copy in own:
        copy.wait_recv()
    for g in mains:
        g.along_first()
    for g in mains:
        g.plane(0)
    for copy in crossed:
        copy.wait_recv()
    lifted = [mail.post(extra.at[:, y, z, x], extra.at[:, y, z, x], {Z: fold(z + d)}) for d in (1, N - 1, 2)]
    for g in mains:
        g.relay_first()
    for g in mains:
        g.plane(N - 1)
        g.plane(1)
    for g in mains:
        g.relay_second(0)
    for g in mains:
        g.far_first()
        g.plane(2)
    for copy in lifted:
        copy.wait_recv()
    for g in mains:
        g.relay_second(1)
    for g in mains:
        g.relay_second(2)
    for g in extras:
        g.along_first()
    for g in extras:
        g.plane(0)
    for g in mains:
        g.relay_second(3)
    for g in mains:
        g.finish()
    load.wait()

    to_sibling = mail.post(
        tokens.at[:, :, :, :, share_of(half, 1 - core)], sibling.at[...], other
    )

    block = group // 2

    def score(k, _):
        rows = tokens[pl.ds(2 * k, 2)].reshape(block, width)
        scores[k] = lax.dot_general(
            embedding[...], rows, (((1,), (1,)), ((), ())), preferred_element_type=F32
        )
        return _

    lax.fori_loop(0, 2, score, 0)

    for g in extras:
        g.relay_first()

    def cap(w, carry):
        total, target = carry
        rows = pl.ds(pl.multiple_of(w * 32, 32), 32)
        raw = jnp.concatenate([scores[0, rows], scores[1, rows]], axis=1)
        capped = softcap * jnp.tanh(raw / softcap)
        scores[0, rows] = capped[:, :block]
        scores[1, rows] = capped[:, block:]
        allowed, onehot = masks(words[pl.ds(w, 1)], targets[...], vocab_start + w * 32)
        total += jnp.where(allowed, jnp.exp(capped), 0.0).reshape(4, 8, group).sum(axis=0)
        target += jnp.where(onehot, capped, 0.0).reshape(4, 8, group).sum(axis=0)
        return total, target

    zero = jnp.zeros((8, group), F32)
    total, target = lax.fori_loop(0, vocab_local // 32, cap, (zero, zero))
    total = total.sum(axis=0, keepdims=True)
    target = target.sum(axis=0, keepdims=True)
    for step, axis in enumerate((X, Y, Z)):
        me = at[axis]
        sums[step, me, 0:1] = total
        sums[step, me, 1:2] = target
        swaps = [
            mail.post(sums.at[step, me], sums.at[step, me], {axis: fold(me + d)}) for d in range(1, N)
        ]
        for copy in swaps:
            copy.wait_recv()
        both = sums[step].sum(axis=0)
        total, target = both[0:1], both[1:2]
    log_total = jnp.log(total)
    loss[...] = log_total - target

    def differentiate(k, _):
        rows = pl.ds(pl.multiple_of(k * 128, 128), 128)
        capped = jnp.concatenate([scores[0, rows], scores[1, rows]], axis=1)
        allowed, onehot = masks(words[pl.ds(4 * k, 4)], targets[...], vocab_start + k * 128)
        probability = jnp.where(allowed, jnp.exp(capped - log_total), 0.0)
        slope = 1.0 - jnp.square(capped / softcap)
        value = (probability - jnp.where(onehot, 1.0, 0.0)) * slope
        dlogits[0, rows] = value.astype(BF16)
        by_token[:, rows] = value.T.astype(BF16)
        return _

    for k in range(vocab_local // 128):
        differentiate(k, 0)

    around = mail.post(dlogits.at[0], dlogits.at[2], partner)
    beside = mail.post(dlogits.at[0], dlogits.at[1], other)

    tile = lane // 3

    def product(k):
        def piece(j, _):
            source = pl.ds(pl.multiple_of(k * lane + j * tile, 128), tile)
            columns = pl.ds(pl.multiple_of(j * tile, 128), tile)
            value = jnp.dot(by_token[...], embedding[:, source], preferred_element_type=F32)
            part[k, :, :, :, :, columns] = value.reshape(N, N, N, ROWS, tile)
            return _

        lax.fori_loop(0, 3, piece, 0)

    lanes = []
    for k, (first, second) in enumerate(((X, Y), (X, Y), (Y, X), (Y, X))):
        boxes = [b.at[k] for b in (send1, recv1, mid, send2, recv2, last, send3, recv3)]
        lanes.append(
            Reduce(mail, part.at[k], boxes, at, first, second, hidden_grad, pl.ds(k * lane, lane))
        )
    early, late = (lanes[0], lanes[2]), (lanes[1], lanes[3])

    def grad(k, source, begin):
        def piece(j, _):
            columns = pl.ds(pl.multiple_of(j * tile, 128), tile)
            value = jnp.dot(
                dlogits[k], source(j).reshape(group, tile), preferred_element_type=F32
            )
            if begin:
                embed_grad[:, columns] = value
            else:
                embed_grad[:, columns] += value
            return _

        lax.fori_loop(0, 3, piece, 0)

    def columns_of(j):
        return pl.ds(pl.multiple_of(j * tile, 128), tile)

    def own_columns(j):
        return pl.ds(pl.multiple_of((2 * half + core) * share + j * tile, 128), tile)

    product(0)
    lanes[0].open1()
    product(2)
    lanes[2].open1()
    product(1)
    product(3)
    for r in early:
        r.relay1()
    for r in late:
        r.open1()
    grad(0, lambda j: tokens[:, :, :, :, own_columns(j)], True)
    for g in extras:
        g.plane(N - 1)
        g.plane(1)
    for g in extras:
        g.relay_second(0)
    for g in extras:
        g.far_first()
        g.plane(2)
    for r in early:
        r.open2()
    for r in late:
        r.relay1()
    beside.wait_recv()
    to_sibling.wait_recv()
    grad(1, lambda j: sibling[:, :, :, :, columns_of(j)], False)
    for r in early:
        r.relay2()
    for g in extras:
        g.relay_second(1)
        g.relay_second(2)
        g.relay_second(3)
    around.wait_recv()
    passed = mail.post(dlogits.at[2], dlogits.at[3], other)
    for r in late:
        r.open2()
    for r in early:
        r.open3()
    for r in late:
        r.relay2()
    for g in extras:
        g.finish()
    grad(2, lambda j: extra[0, :, :, :, :, columns_of(j)], False)
    for r in late:
        r.open3()
    passed.wait_recv()
    grad(3, lambda j: extra[1, :, :, :, :, columns_of(j)], False)
    for r in early + late:
        r.finish()
    mail.close()


def on_device(hidden, embedding, targets, grammar_bits):
    rows, width = hidden.shape
    vocab_local = embedding.shape[0]
    group = targets.shape[0]
    lane = width // 4
    vmem = pl.BlockSpec(memory_space=pltpu.VMEM)
    blocks = (N, N, N, ROWS)
    loss, hidden_grad, embed_grad = pl.pallas_call(
        kernel,
        out_shape=(
            jax.ShapeDtypeStruct((1, group), F32),
            jax.ShapeDtypeStruct((rows, width), F32),
            jax.ShapeDtypeStruct((vocab_local, lane), F32),
        ),
        in_specs=[vmem, vmem, vmem, pl.BlockSpec(memory_space=pl.ANY)],
        out_specs=(vmem, vmem, vmem),
        scratch_shapes=[
            pltpu.VMEM(blocks + (width,), BF16),
            pltpu.VMEM((2,) + blocks + (lane,), BF16),
            pltpu.VMEM(blocks + (lane,), BF16),
            pltpu.VMEM((vocab_local, width), BF16),
            pltpu.VMEM((2, vocab_local, group // 2), F32),
            pltpu.VMEM((4, vocab_local, group), BF16),
            pltpu.VMEM((group, vocab_local), BF16),
            pltpu.VMEM((4,) + blocks + (lane,), F32),
            pltpu.VMEM((3, N, 2, group), F32),
            pltpu.VMEM((4, 6, N, 2, ROWS, lane), BF16),
            pltpu.VMEM((4, 6, N, 2, ROWS, lane), BF16),
            pltpu.VMEM((4, N, N, ROWS, lane), F32),
            pltpu.VMEM((4, 6, 2, ROWS, lane), F32),
            pltpu.VMEM((4, 6, 2, ROWS, lane), F32),
            pltpu.VMEM((4, N, ROWS, lane), F32),
            pltpu.VMEM((4, N - 1, ROWS, lane), BF16),
            pltpu.VMEM((4, N - 1, ROWS, lane), BF16),
            pltpu.SemaphoreType.DMA,
            pltpu.SemaphoreType.DMA((170,)),
            pltpu.SemaphoreType.DMA((170,)),
        ],
        compiler_params=pltpu.CompilerParams(
            collective_id=0, has_side_effects=True, vmem_limit_bytes=67043328
        ),
        name="fused",
    )(hidden, grammar_bits.T, targets[None, :], embedding)
    return loss[0], hidden_grad, embed_grad


def solution(mesh):
    split = Mesh(mesh.devices.reshape(2, 2, 4, 4, 4), AXES)
    return jax.shard_map(
        on_device,
        mesh=split,
        in_specs=(P(AXES, None), P(VOCAB, None), P(DP), P(DP, VOCAB)),
        out_specs=(P(DP), P(AXES, None), P(VOCAB, DP)),
        check_vma=False,
    )
```

```python
import functools

import jax
import jax.numpy as jnp
from jax import lax
from jax.experimental import pallas as pl
from jax.experimental.pallas import tpu as pltpu
from jax.sharding import Mesh
from jax.sharding import PartitionSpec as P

AXES = ("dp_0", "dp_1", "vocab_0", "vocab_1", "vocab_2")
VOCAB = ("vocab_0", "vocab_1", "vocab_2")
DP = ("dp_0", "dp_1")
HALF, CORE, Y, Z, X = AXES
MESH = pl.DeviceIdType.MESH
N = 4
ROWS = 8
LANES = 3
softcap = 30.0
F32, BF16 = jnp.float32, jnp.bfloat16


def fold(k):
    return lax.rem(k, N)


def masks(words, targets, first_id):
    rows = 32 * words.shape[0]
    bit = lax.broadcasted_iota(jnp.int32, (32, words.shape[1]), 0)
    spread = [jnp.right_shift(words[k : k + 1], bit) & 1 for k in range(words.shape[0])]
    unpacked = spread[0] if len(spread) == 1 else jnp.concatenate(spread, axis=0)
    ids = first_id + lax.broadcasted_iota(jnp.int32, (rows, words.shape[1]), 0)
    onehot = ids == targets
    return (unpacked == 1) | onehot, onehot


class Mail:
    def __init__(self, send_sem, recv_sem):
        self.send_sem, self.recv_sem = send_sem, recv_sem
        self.count = 0
        self.sent = []

    def describe(self, src, dst, device, send, recv):
        return pltpu.make_async_remote_copy(
            src_ref=src,
            dst_ref=dst,
            send_sem=self.send_sem.at[send],
            recv_sem=self.recv_sem.at[recv],
            device_id=device,
            device_id_type=MESH,
        )

    def start(self, copy):
        copy.start()
        self.sent.append(copy)
        return copy

    def post(self, src, dst, device):
        k = self.count
        self.count += 1
        return self.start(self.describe(src, dst, device, k, k))

    def post_each(self, src, dst, axis, me, steps):
        base = self.count - 1
        self.count += N - 1
        for d in steps:
            self.start(self.describe(src, dst, {axis: fold(me + d)}, base + d, base + N - d))
        return [self.describe(src, dst, {axis: fold(me + d)}, base + d, base + d) for d in steps]

    def close(self):
        for copy in self.sent:
            copy.wait_send()


class Gather:
    def __init__(self, mail, view, at, first, second, span):
        self.mail, self.view, self.span = mail, view, span
        self.first, self.second = first, second
        self.u, self.v = at[first], at[second]
        self.relays = []
        self.planes = {}

    def ref(self, u, v, piece):
        y, x = (u, v) if self.first == Y else (v, u)
        return self.view(y, x, self.span[piece])

    def both(self, axis, ref, src=None):
        k = self.u if axis == self.first else self.v
        return [
            self.mail.post(ref if src is None else src, ref, {axis: fold(k + d)}) for d in (1, N - 1)
        ]

    def along_first(self, src=None):
        self.near = self.both(self.first, self.ref(self.u, self.v, 0), src)

    def plane(self, d, src=None):
        self.planes[d] = self.both(self.second, self.ref(fold(self.u + d), self.v, 0), src)

    def relay_first(self):
        before, after = fold(self.u + N - 1), fold(self.u + 1)
        self.near[0].wait_recv()
        low = self.ref(before, self.v, 1)
        self.far = [self.mail.post(low, low, {self.first: after})]
        self.near[1].wait_recv()
        high = self.ref(after, self.v, 2)
        self.far.append(self.mail.post(high, high, {self.first: before}))

    def far_first(self):
        for copy in self.far:
            copy.wait_recv()

    def relay_second(self, d):
        before, after = fold(self.v + N - 1), fold(self.v + 1)
        p = fold(self.u + d)
        self.planes[d][0].wait_recv()
        low = self.ref(p, before, 1)
        self.relays.append(self.mail.post(low, low, {self.second: after}))
        self.planes[d][1].wait_recv()
        high = self.ref(p, after, 2)
        self.relays.append(self.mail.post(high, high, {self.second: before}))

    def finish(self):
        for copy in self.relays:
            copy.wait_recv()


def advance(gathers, step, sources=None):
    if step == 0:
        for k, g in enumerate(gathers):
            g.along_first(sources and sources[k])
        for k, g in enumerate(gathers):
            g.plane(0, sources and sources[k])
    elif step == 1:
        for g in gathers:
            g.relay_first()
            g.plane(N - 1)
            g.plane(1)
    elif step == 2:
        for g in gathers:
            g.relay_second(0)
        for g in gathers:
            g.far_first()
            g.plane(2)
    elif step == 3:
        for g in gathers:
            g.relay_second(N - 1)
            g.relay_second(1)
    elif step == 4:
        for g in gathers:
            g.relay_second(2)
    else:
        for g in gathers:
            g.finish()


class Reduce:
    def __init__(self, mail, part, boxes, at, first, second, out, columns):
        self.mail, self.part, self.at = mail, part, at
        self.send1, self.recv1, self.mid, self.send2, self.recv2, self.last, self.send3, self.recv3 = boxes
        self.first, self.second = first, second
        self.u, self.w = at[first], at[second]
        self.out, self.columns = out, columns

    def partial(self, u, w, start):
        y, x = (w, u) if self.first == X else (u, w)
        return self.part[y, pl.ds(start, 2), x]

    def post1(self, k, d):
        return self.mail.post(self.send1.at[k], self.recv1.at[k], {self.first: fold(self.u + d)})

    def post2(self, k, d):
        return self.mail.post(self.send2.at[k], self.recv2.at[k], {self.second: fold(self.w + d)})

    def open1(self):
        self.one = []
        plan = ((2, 0, 1), (2, 2, N - 1), (1, 2, 1), (N - 1, 0, N - 1))
        for k, (to, start, d) in enumerate(plan):
            u = fold(self.u + to)

            def stage(w, _):
                self.send1[k, w] = self.partial(u, w, start).astype(BF16)
                return _

            lax.fori_loop(0, N, stage, 0)
            self.one.append(self.post1(k, d))

    def relay1(self):
        for k, to, start in ((0, 1, 0), (1, N - 1, 2)):
            self.one[k].wait_recv()
            u = fold(self.u + to)

            def stage(w, _):
                total = self.partial(u, w, start) + self.recv1[k, w].astype(F32)
                self.send1[4 + k, w] = total.astype(BF16)
                return _

            lax.fori_loop(0, N, stage, 0)
            self.one.append(self.post1(4 + k, to))

    def open2(self):
        for k in (2, 3, 4, 5):
            self.one[k].wait_recv()

        def total(w, _):
            self.mid[w, 0:2] = (
                self.partial(self.u, w, 0) + self.recv1[3, w].astype(F32) + self.recv1[4, w].astype(F32)
            )
            self.mid[w, 2:4] = (
                self.partial(self.u, w, 2) + self.recv1[2, w].astype(F32) + self.recv1[5, w].astype(F32)
            )
            return _

        lax.fori_loop(0, N, total, 0)
        self.two = []
        plan = ((2, 0, 1), (2, 2, N - 1), (1, 2, 1), (N - 1, 0, N - 1))
        for k, (to, start, d) in enumerate(plan):
            self.send2[k] = self.mid[fold(self.w + to), start : start + 2].astype(self.send2.dtype)
            self.two.append(self.post2(k, d))

    def relay2(self):
        for k, to, start in ((0, 1, 0), (1, N - 1, 2)):
            self.two[k].wait_recv()
            total = self.mid[fold(self.w + to), start : start + 2] + self.recv2[k].astype(F32)
            self.send2[4 + k] = total.astype(self.send2.dtype)
            self.two.append(self.post2(4 + k, to))

    def open3(self):
        for k in (2, 3, 4, 5):
            self.two[k].wait_recv()
        self.last[0:2] = self.mid[self.w, 0:2] + self.recv2[3].astype(F32) + self.recv2[4].astype(F32)
        self.last[2:4] = self.mid[self.w, 2:4] + self.recv2[2].astype(F32) + self.recv2[5].astype(F32)
        self.three = []
        for d in (2, 1, N - 1):
            z = fold(self.at[Z] + d)
            self.send3[d - 1] = self.last[z].astype(BF16)
            self.three.append(self.mail.post(self.send3.at[d - 1], self.recv3.at[d - 1], {Z: z}))

    def finish(self):
        total = self.last[self.at[Z]]
        for copy in self.three:
            copy.wait_recv()
        for d in range(1, N):
            total += self.recv3[d - 1].astype(F32)
        self.out[:, self.columns] = total


def kernel(
    hidden, words, targets, embedding_hbm,
    loss, hidden_grad, embed_grad,
    tokens, extra, sibling, embedding, scores, slopes, picks, slopes_t, picks_t, dlogits, by_token, part, plane_sums, depth_sums,
    send1, recv1, mid, send2, recv2, last, send3, recv3,
    load_sem, send_sem, recv_sem,
):
    at = {a: lax.axis_index(a) for a in AXES}
    half, core, y, z, x = (at[a] for a in AXES)
    width = hidden.shape[1]
    vocab_local = embedding.shape[0]
    group = tokens.shape[0] * tokens.shape[1] * tokens.shape[2] * ROWS
    color, share, lane = width // 2, width // 4, width // (2 * LANES)
    partner = {HALF: 1 - half}
    across = {HALF: 1 - half, CORE: 1 - core}
    other = {CORE: 1 - core}
    vocab_start = ((y * N + z) * N + x) * vocab_local

    load = pltpu.make_async_copy(embedding_hbm, embedding, load_sem)
    load.start()
    barrier = pltpu.get_barrier_semaphore()
    plane_peers = [(i, j) for i in range(N) for j in range(N) if i or j]
    greeted = [{Y: fold(y + i), X: fold(x + j)} for i, j in plane_peers]
    greeted += [{Z: fold(z + d)} for d in range(1, N)] + [partner, across, other]
    for device in greeted:
        pl.semaphore_signal(barrier, inc=1, device_id=device, device_id_type=MESH)
    pl.semaphore_wait(barrier, len(greeted))

    mail = Mail(send_sem, recv_sem)
    inner = z * (N - 1 - z) // 2
    nearest, middle = 1 + 2 * (z // 2), 2 + inner * (3 - 2 * z)
    order = (nearest, middle, 6 - nearest - middle)
    own = mail.post_each(hidden, tokens.at[y, z, x], Z, z, order)

    def share_of(h, c):
        return pl.ds(pl.multiple_of((2 * h + c) * share, 128), share)

    def slot(k, start, size):
        half_size = size // 2
        zs = pl.ds(k, 1)
        return (
            (zs, pl.ds(start, size)),
            (zs, pl.ds(start, half_size)),
            (zs, pl.ds(start + half_size, half_size)),
        )

    def main_view(yy, xx, piece):
        return tokens.at[yy, piece[0], xx, :, piece[1]]

    def extra_view(k):
        return lambda yy, xx, piece: extra.at[k, yy, piece[0], xx]

    def main_pair(k):
        return [
            Gather(mail, main_view, at, Y, X, slot(k, 0, color)),
            Gather(mail, main_view, at, X, Y, slot(k, color, color)),
        ]

    tokens[y, z, x] = hidden[...]
    mains = [main_pair(z)] + [main_pair(fold(z + d)) for d in order]
    advance(mains[0], 0)
    crossed = [
        mail.post(hidden.at[:, share_of(1 - half, core)], extra.at[0, y, z, x], partner),
        mail.post(hidden.at[:, share_of(1 - half, 1 - core)], extra.at[1, y, z, x], across),
    ]
    depth = ((pl.ds(0, N),), (pl.ds(0, 2),), (pl.ds(2, 2),))
    extras = [
        Gather(mail, extra_view(0), at, Y, X, depth),
        Gather(mail, extra_view(1), at, X, Y, depth),
    ]
    advance(mains[0], 1)
    own[0].wait_recv()
    advance(mains[1], 0)
    advance(mains[0], 2)
    own[1].wait_recv()
    advance(mains[2], 0)
    advance(mains[1], 1)
    own[2].wait_recv()
    advance(mains[3], 0)
    advance(mains[0], 3)
    advance(mains[2], 1)
    advance(mains[1], 2)
    for copy in crossed:
        copy.wait_recv()
    lifted = mail.post_each(extra.at[:, y, z, x], extra.at[:, y, z, x], Z, z, order)
    advance(mains[3], 1)
    advance(mains[2], 2)
    advance(mains[0], 4)
    advance(mains[1], 3)
    advance(mains[3], 2)
    advance(mains[2], 3)
    advance(mains[1], 4)
    advance(mains[3], 3)
    advance(mains[2], 4)
    for copy in lifted:
        copy.wait_recv()
    advance(mains[3], 4)
    advance(extras, 0)
    for pair in mains:
        advance(pair, 5)
    load.wait()

    to_sibling = mail.post(
        tokens.at[:, :, :, :, share_of(half, 1 - core)], sibling.at[...], other
    )

    block = group // 2

    def score(k):
        rows = tokens[pl.ds(2 * k, 2)].reshape(block, width)
        scores[k] = lax.dot_general(
            embedding[...], rows, (((1,), (1,)), ((), ())), preferred_element_type=F32
        )

    score(0)
    for g in extras:
        g.relay_first()
    score(1)

    def cap(w, carry):
        total, target = carry
        rows = pl.ds(pl.multiple_of(w * 32, 32), 32)
        raw = jnp.concatenate([scores[0, rows], scores[1, rows]], axis=1)
        capped = softcap * jnp.tanh(raw / softcap)
        allowed, onehot = masks(words[pl.ds(w, 1)], targets[...], vocab_start + w * 32)
        weight = jnp.where(allowed, jnp.exp(capped), 0.0)
        total += weight.reshape(4, 8, group).sum(axis=0)
        target += jnp.where(onehot, capped, 0.0).reshape(4, 8, group).sum(axis=0)
        slope = 1.0 - jnp.square(capped / softcap)
        slopes[rows] = weight * slope
        picks[rows] = jnp.where(onehot, slope, 0.0)
        return total, target

    zero = jnp.zeros((8, group), F32)
    total, target = lax.fori_loop(0, vocab_local // 32, cap, (zero, zero))
    total = total.sum(axis=0, keepdims=True)
    target = target.sum(axis=0, keepdims=True)

    def swap(sums, me, peers):
        sums[me, 0:1] = total
        sums[me, 1:2] = target
        return [mail.post(sums.at[me], sums.at[me], device) for device in peers]

    def summed(sums, copies):
        for copy in copies:
            copy.wait_recv()
        both = sums[...].sum(axis=0)
        return both[0:1], both[1:2]

    def turn(k):
        rows = pl.ds(k * 128, 128)
        slopes_t[:, rows] = slopes[rows].T
        picks_t[:, rows] = picks[rows].T

    copies = swap(plane_sums, y * N + x, [{Y: fold(y + i), X: fold(x + j)} for i, j in plane_peers])
    for g in extras:
        g.plane(N - 1)
        g.plane(1)
    for k in range(vocab_local // 128):
        turn(k)
    total, target = summed(plane_sums, copies)
    copies = swap(depth_sums, z, [{Z: fold(z + d)} for d in range(1, N)])
    advance(extras, 2)
    total, target = summed(depth_sums, copies)
    log_total = jnp.log(total)
    loss[...] = log_total - target
    inverse = 1.0 / total
    inverse_t = jnp.broadcast_to(inverse, (128, group)).T

    for k in range(vocab_local // 128):
        columns = pl.ds(k * 128, 128)
        by_token[:, columns] = (slopes_t[:, columns] * inverse_t - picks_t[:, columns]).astype(BF16)

    def by_vocabulary(k, _):
        rows = pl.ds(pl.multiple_of(k * 32, 32), 32)
        dlogits[0, rows] = (slopes[rows] * inverse - picks[rows]).astype(BF16)
        return _

    tile = share // 3

    def product(k):
        step = lane // 2

        def piece(j, _):
            source = pl.ds(pl.multiple_of(k * lane + j * step, 128), step)
            columns = pl.ds(pl.multiple_of(j * step, 128), step)
            value = jnp.dot(by_token[...], embedding[:, source], preferred_element_type=F32)
            part[k, :, :, :, :, columns] = value.reshape(N, N, N, ROWS, step)
            return _

        lax.fori_loop(0, 2, piece, 0)

    def reducer(k, first, second):
        boxes = [b.at[k] for b in (send1, recv1, mid, send2, recv2, last, send3, recv3)]
        return Reduce(mail, part.at[k], boxes, at, first, second, hidden_grad, pl.ds(k * lane, lane))

    lanes = [(k, k + LANES) for k in range(LANES)]
    pairs = [(reducer(i, X, Y), reducer(j, Y, X)) for i, j in lanes]

    def open1(k):
        for i, r in zip(lanes[k], pairs[k]):
            product(i)
            r.open1()

    def run(k, *names):
        for name in names:
            for r in pairs[k]:
                getattr(r, name)()

    def grad(k, source, begin):
        def piece(j, _):
            columns = pl.ds(pl.multiple_of(j * tile, 128), tile)
            value = jnp.dot(
                dlogits[k], source(j).reshape(group, tile), preferred_element_type=F32
            )
            if begin:
                embed_grad[:, columns] = value
            else:
                embed_grad[:, columns] += value
            return _

        lax.fori_loop(0, 3, piece, 0)

    def columns_of(j):
        return pl.ds(pl.multiple_of(j * tile, 128), tile)

    def own_columns(j):
        return pl.ds(pl.multiple_of((2 * half + core) * share + j * tile, 128), tile)

    open1(0)
    lax.fori_loop(0, vocab_local // 32, by_vocabulary, 0)
    around = mail.post(dlogits.at[0], dlogits.at[2], partner)
    beside = mail.post(dlogits.at[0], dlogits.at[1], other)
    run(0, "relay1")
    open1(1)
    grad(0, lambda j: tokens[:, :, :, :, own_columns(j)], True)
    run(1, "relay1")
    run(0, "open2")
    open1(2)
    run(0, "relay2")
    run(2, "relay1")
    run(1, "open2")
    run(0, "open3")
    beside.wait_recv()
    to_sibling.wait_recv()
    grad(1, lambda j: sibling[:, :, :, :, columns_of(j)], False)
    run(2, "open2")
    advance(extras, 3)
    run(1, "relay2")
    around.wait_recv()
    passed = mail.post(dlogits.at[2], dlogits.at[3], other)
    run(2, "relay2")
    advance(extras, 4)
    run(1, "open3")
    run(2, "open3")
    advance(extras, 5)
    grad(2, lambda j: extra[0, :, :, :, :, columns_of(j)], False)
    passed.wait_recv()
    grad(3, lambda j: extra[1, :, :, :, :, columns_of(j)], False)
    for k in range(LANES):
        run(k, "finish")
    mail.close()


def write_out(loss, hidden_grad, embed_grad, loss_out, hidden_out, embed_out, sem):
    pairs = ((hidden_grad, hidden_out), (embed_grad, embed_out))
    copies = [pltpu.make_async_copy(a, b, sem.at[k]) for k, (a, b) in enumerate(pairs)]
    for copy in copies:
        copy.start()
    loss_out[...] = loss[0]
    for copy in copies:
        copy.wait()


def on_device(hidden, embedding, targets, grammar_bits):
    rows, width = hidden.shape
    vocab_local = embedding.shape[0]
    group = targets.shape[0]
    share, lane, lanes = width // 4, width // (2 * LANES), 2 * LANES
    vmem = pl.BlockSpec(memory_space=pltpu.VMEM)
    blocks = (N, N, N, ROWS)
    hbm = pl.BlockSpec(memory_space=pltpu.HBM)
    results = pl.pallas_call(
        kernel,
        out_shape=(
            jax.ShapeDtypeStruct((1, group), F32),
            jax.ShapeDtypeStruct((rows, width), F32),
            jax.ShapeDtypeStruct((vocab_local, share), F32),
        ),
        in_specs=[vmem, vmem, vmem, hbm],
        out_specs=(vmem, vmem, vmem),
        scratch_shapes=[
            pltpu.VMEM(blocks + (width,), BF16),
            pltpu.VMEM((2,) + blocks + (share,), BF16),
            pltpu.VMEM(blocks + (share,), BF16),
            pltpu.VMEM((vocab_local, width), BF16),
            pltpu.VMEM((2, vocab_local, group // 2), F32),
            pltpu.VMEM((vocab_local, group), F32),
            pltpu.VMEM((vocab_local, group), F32),
            pltpu.VMEM((group, vocab_local), F32),
            pltpu.VMEM((group, vocab_local), F32),
            pltpu.VMEM((4, vocab_local, group), BF16),
            pltpu.VMEM((group, vocab_local), BF16),
            pltpu.VMEM((lanes,) + blocks + (lane,), F32),
            pltpu.VMEM((N * N, 2, group), F32),
            pltpu.VMEM((N, 2, group), F32),
            pltpu.VMEM((lanes, 6, N, 2, ROWS, lane), BF16),
            pltpu.VMEM((lanes, 6, N, 2, ROWS, lane), BF16),
            pltpu.VMEM((lanes, N, N, ROWS, lane), F32),
            pltpu.VMEM((lanes, 6, 2, ROWS, lane), F32),
            pltpu.VMEM((lanes, 6, 2, ROWS, lane), F32),
            pltpu.VMEM((lanes, N, ROWS, lane), F32),
            pltpu.VMEM((lanes, N - 1, ROWS, lane), BF16),
            pltpu.VMEM((lanes, N - 1, ROWS, lane), BF16),
            pltpu.SemaphoreType.DMA,
            pltpu.SemaphoreType.DMA((340,)),
            pltpu.SemaphoreType.DMA((340,)),
        ],
        compiler_params=pltpu.CompilerParams(
            collective_id=0, has_side_effects=True, vmem_limit_bytes=50 * 1024 * 1024
        ),
        name="fused",
    )(hidden, grammar_bits.T, targets[None, :], embedding)
    return pl.pallas_call(
        write_out,
        out_shape=(
            jax.ShapeDtypeStruct((group,), F32),
            jax.ShapeDtypeStruct((rows, width), F32),
            jax.ShapeDtypeStruct((vocab_local, share), F32),
        ),
        in_specs=[vmem, vmem, vmem],
        out_specs=(vmem, hbm, hbm),
        scratch_shapes=[pltpu.SemaphoreType.DMA((2,))],
        compiler_params=pltpu.CompilerParams(vmem_limit_bytes=8 * 1024 * 1024),
        name="write_out",
    )(*results)


def solution(mesh):
    split = Mesh(mesh.devices.reshape(2, 2, 4, 4, 4), AXES)
    return jax.shard_map(
        on_device,
        mesh=split,
        in_specs=(P(AXES, None), P(VOCAB, None), P(DP), P(DP, VOCAB)),
        out_specs=(P(DP), P(AXES, None), P(VOCAB, DP)),
        check_vma=False,
    )
```

```python
import functools

import jax
import jax.numpy as jnp
from jax import lax
from jax.experimental import pallas as pl
from jax.experimental.pallas import tpu as pltpu
from jax.sharding import Mesh
from jax.sharding import PartitionSpec as P

AXES = ("dp_0", "dp_1", "vocab_0", "vocab_1", "vocab_2")
VOCAB = ("vocab_0", "vocab_1", "vocab_2")
DP = ("dp_0", "dp_1")
HALF, CORE, Y, Z, X = AXES
MESH = pl.DeviceIdType.MESH
N = 4
ROWS = 8
LANES = 3
softcap = 30.0
F32, BF16 = jnp.float32, jnp.bfloat16


def fold(k):
    return lax.rem(k, N)


def masks(words, targets, first_id):
    rows = 32 * words.shape[0]
    bit = lax.broadcasted_iota(jnp.int32, (32, words.shape[1]), 0)
    spread = [jnp.right_shift(words[k : k + 1], bit) & 1 for k in range(words.shape[0])]
    unpacked = spread[0] if len(spread) == 1 else jnp.concatenate(spread, axis=0)
    ids = first_id + lax.broadcasted_iota(jnp.int32, (rows, words.shape[1]), 0)
    onehot = ids == targets
    return (unpacked == 1) | onehot, onehot


class Mail:
    def __init__(self, send_sem, recv_sem):
        self.send_sem, self.recv_sem = send_sem, recv_sem
        self.count = 0
        self.sent = []

    def describe(self, src, dst, device, send, recv):
        return pltpu.make_async_remote_copy(
            src_ref=src,
            dst_ref=dst,
            send_sem=self.send_sem.at[send],
            recv_sem=self.recv_sem.at[recv],
            device_id=device,
            device_id_type=MESH,
        )

    def start(self, copy):
        copy.start()
        self.sent.append(copy)
        return copy

    def post(self, src, dst, device):
        k = self.count
        self.count += 1
        return self.start(self.describe(src, dst, device, k, k))

    def post_each(self, src, dst, axis, me, steps):
        base = self.count - 1
        self.count += N - 1
        for d in steps:
            self.start(self.describe(src, dst, {axis: fold(me + d)}, base + d, base + N - d))
        return [self.describe(src, dst, {axis: fold(me + d)}, base + d, base + d) for d in steps]

    def close(self):
        for copy in self.sent:
            copy.wait_send()


class Gather:
    def __init__(self, mail, view, at, first, second, span):
        self.mail, self.view, self.span = mail, view, span
        self.first, self.second = first, second
        self.u, self.v = at[first], at[second]
        self.relays = []
        self.planes = {}

    def ref(self, u, v, piece):
        y, x = (u, v) if self.first == Y else (v, u)
        return self.view(y, x, self.span[piece])

    def both(self, axis, ref, src=None):
        k = self.u if axis == self.first else self.v
        return [
            self.mail.post(ref if src is None else src, ref, {axis: fold(k + d)}) for d in (1, N - 1)
        ]

    def along_first(self, src=None):
        self.near = self.both(self.first, self.ref(self.u, self.v, 0), src)

    def plane(self, d, src=None):
        self.planes[d] = self.both(self.second, self.ref(fold(self.u + d), self.v, 0), src)

    def relay_first(self):
        before, after = fold(self.u + N - 1), fold(self.u + 1)
        self.near[0].wait_recv()
        low = self.ref(before, self.v, 1)
        self.far = [self.mail.post(low, low, {self.first: after})]
        self.near[1].wait_recv()
        high = self.ref(after, self.v, 2)
        self.far.append(self.mail.post(high, high, {self.first: before}))

    def far_first(self):
        for copy in self.far:
            copy.wait_recv()

    def relay_second(self, d):
        before, after = fold(self.v + N - 1), fold(self.v + 1)
        p = fold(self.u + d)
        self.planes[d][0].wait_recv()
        low = self.ref(p, before, 1)
        self.relays.append(self.mail.post(low, low, {self.second: after}))
        self.planes[d][1].wait_recv()
        high = self.ref(p, after, 2)
        self.relays.append(self.mail.post(high, high, {self.second: before}))

    def finish(self):
        for copy in self.relays:
            copy.wait_recv()


def advance(gathers, step, sources=None):
    if step == 0:
        for k, g in enumerate(gathers):
            g.along_first(sources and sources[k])
        for k, g in enumerate(gathers):
            g.plane(0, sources and sources[k])
    elif step == 1:
        for g in gathers:
            g.relay_first()
            g.plane(N - 1)
            g.plane(1)
    elif step == 2:
        for g in gathers:
            g.relay_second(0)
        for g in gathers:
            g.far_first()
            g.plane(2)
    elif step == 3:
        for g in gathers:
            g.relay_second(N - 1)
            g.relay_second(1)
    elif step == 4:
        for g in gathers:
            g.relay_second(2)
    else:
        for g in gathers:
            g.finish()


class Reduce:
    def __init__(self, mail, part, boxes, at, first, second, out, columns):
        self.mail, self.part, self.at = mail, part, at
        self.send1, self.recv1, self.mid, self.send2, self.recv2, self.last, self.send3, self.recv3 = boxes
        self.first, self.second = first, second
        self.u, self.w = at[first], at[second]
        self.out, self.columns = out, columns

    def partial(self, u, w, start):
        y, x = (w, u) if self.first == X else (u, w)
        return self.part[y, pl.ds(start, 2), x]

    def post1(self, k, d):
        return self.mail.post(self.send1.at[k], self.recv1.at[k], {self.first: fold(self.u + d)})

    def post2(self, k, d):
        return self.mail.post(self.send2.at[k], self.recv2.at[k], {self.second: fold(self.w + d)})

    def open1(self):
        self.one = []
        plan = ((2, 0, 1), (2, 2, N - 1), (1, 2, 1), (N - 1, 0, N - 1))
        for k, (to, start, d) in enumerate(plan):
            u = fold(self.u + to)

            def stage(w, _):
                self.send1[k, w] = self.partial(u, w, start).astype(BF16)
                return _

            lax.fori_loop(0, N, stage, 0)
            self.one.append(self.post1(k, d))

    def relay1(self):
        for k, to, start in ((0, 1, 0), (1, N - 1, 2)):
            self.one[k].wait_recv()
            u = fold(self.u + to)

            def stage(w, _):
                total = self.partial(u, w, start) + self.recv1[k, w].astype(F32)
                self.send1[4 + k, w] = total.astype(BF16)
                return _

            lax.fori_loop(0, N, stage, 0)
            self.one.append(self.post1(4 + k, to))

    def open2(self):
        for k in (2, 3, 4, 5):
            self.one[k].wait_recv()

        def total(w, _):
            self.mid[w, 0:2] = (
                self.partial(self.u, w, 0) + self.recv1[3, w].astype(F32) + self.recv1[4, w].astype(F32)
            )
            self.mid[w, 2:4] = (
                self.partial(self.u, w, 2) + self.recv1[2, w].astype(F32) + self.recv1[5, w].astype(F32)
            )
            return _

        lax.fori_loop(0, N, total, 0)
        self.two = []
        plan = ((2, 0, 1), (2, 2, N - 1), (1, 2, 1), (N - 1, 0, N - 1))
        for k, (to, start, d) in enumerate(plan):
            self.send2[k] = self.mid[fold(self.w + to), start : start + 2].astype(self.send2.dtype)
            self.two.append(self.post2(k, d))

    def relay2(self):
        for k, to, start in ((0, 1, 0), (1, N - 1, 2)):
            self.two[k].wait_recv()
            total = self.mid[fold(self.w + to), start : start + 2] + self.recv2[k].astype(F32)
            self.send2[4 + k] = total.astype(self.send2.dtype)
            self.two.append(self.post2(4 + k, to))

    def open3(self):
        for k in (2, 3, 4, 5):
            self.two[k].wait_recv()
        self.last[0:2] = self.mid[self.w, 0:2] + self.recv2[3].astype(F32) + self.recv2[4].astype(F32)
        self.last[2:4] = self.mid[self.w, 2:4] + self.recv2[2].astype(F32) + self.recv2[5].astype(F32)
        self.three = []
        for d in (2, 1, N - 1):
            z = fold(self.at[Z] + d)
            self.send3[d - 1] = self.last[z].astype(BF16)
            self.three.append(self.mail.post(self.send3.at[d - 1], self.recv3.at[d - 1], {Z: z}))

    def finish(self):
        total = self.last[self.at[Z]]
        for copy in self.three:
            copy.wait_recv()
        for d in range(1, N):
            total += self.recv3[d - 1].astype(F32)
        self.out[:, self.columns] = total


def kernel(
    hidden, words, targets, embedding_hbm,
    loss, hidden_grad, embed_grad,
    tokens, extra, sibling, embedding, embedding_t, scores, slopes, picks, slopes_t, picks_t, dlogits, by_token, part, plane_sums, depth_sums,
    send1, recv1, mid, send2, recv2, last, send3, recv3,
    load_sem, send_sem, recv_sem,
):
    at = {a: lax.axis_index(a) for a in AXES}
    half, core, y, z, x = (at[a] for a in AXES)
    width = hidden.shape[1]
    vocab_local = embedding.shape[0]
    group = tokens.shape[0] * tokens.shape[1] * tokens.shape[2] * ROWS
    color, share, lane = width // 2, width // 4, width // (2 * LANES)
    partner = {HALF: 1 - half}
    across = {HALF: 1 - half, CORE: 1 - core}
    other = {CORE: 1 - core}
    vocab_start = ((y * N + z) * N + x) * vocab_local

    load = pltpu.make_async_copy(embedding_hbm, embedding, load_sem)
    load.start()
    barrier = pltpu.get_barrier_semaphore()
    plane_peers = [(i, j) for i in range(N) for j in range(N) if i or j]
    greeted = [{Y: fold(y + i), X: fold(x + j)} for i, j in plane_peers]
    greeted += [{Z: fold(z + d)} for d in range(1, N)] + [partner, across, other]
    for device in greeted:
        pl.semaphore_signal(barrier, inc=1, device_id=device, device_id_type=MESH)
    pl.semaphore_wait(barrier, len(greeted))

    mail = Mail(send_sem, recv_sem)
    inner = z * (N - 1 - z) // 2
    nearest, middle = 1 + 2 * (z // 2), 2 + inner * (3 - 2 * z)
    order = (nearest, middle, 6 - nearest - middle)
    own = mail.post_each(hidden, tokens.at[y, z, x], Z, z, order)

    def share_of(h, c):
        return pl.ds(pl.multiple_of((2 * h + c) * share, 128), share)

    def slot(k, start, size):
        half_size = size // 2
        zs = pl.ds(k, 1)
        return (
            (zs, pl.ds(start, size)),
            (zs, pl.ds(start, half_size)),
            (zs, pl.ds(start + half_size, half_size)),
        )

    def main_view(yy, xx, piece):
        return tokens.at[yy, piece[0], xx, :, piece[1]]

    def extra_view(k):
        return lambda yy, xx, piece: extra.at[k, yy, piece[0], xx]

    def main_pair(k):
        return [
            Gather(mail, main_view, at, Y, X, slot(k, 0, color)),
            Gather(mail, main_view, at, X, Y, slot(k, color, color)),
        ]

    tokens[y, z, x] = hidden[...]
    mains = [main_pair(z)] + [main_pair(fold(z + d)) for d in order]
    def flip(part):
        blocks = width // 256

        def piece(k, _):
            span = pl.ds(pl.multiple_of((part * blocks + k) * 128, 128), 128)
            embedding_t[span, :] = embedding[:, span].T
            return _

        lax.fori_loop(0, blocks, piece, 0)

    advance(mains[0], 0)
    crossed = [
        mail.post(hidden.at[:, share_of(1 - half, core)], extra.at[0, y, z, x], partner),
        mail.post(hidden.at[:, share_of(1 - half, 1 - core)], extra.at[1, y, z, x], across),
    ]
    depth = ((pl.ds(0, N),), (pl.ds(0, 2),), (pl.ds(2, 2),))
    extras = [
        Gather(mail, extra_view(0), at, Y, X, depth),
        Gather(mail, extra_view(1), at, X, Y, depth),
    ]
    advance(mains[0], 1)
    own[0].wait_recv()
    advance(mains[1], 0)
    advance(mains[0], 2)
    advance(mains[1], 1)
    load.wait()
    flip(0)
    own[1].wait_recv()
    advance(mains[2], 0)
    advance(mains[0], 3)
    own[2].wait_recv()
    advance(mains[3], 0)
    advance(mains[1], 2)
    for copy in crossed:
        copy.wait_recv()
    lifted = mail.post_each(extra.at[:, y, z, x], extra.at[:, y, z, x], Z, z, order)
    advance(mains[2], 1)
    advance(mains[0], 4)
    advance(mains[3], 1)
    advance(mains[1], 3)
    flip(1)
    advance(mains[2], 2)
    advance(mains[1], 4)
    advance(mains[3], 2)
    advance(mains[2], 3)
    advance(mains[3], 3)
    advance(mains[2], 4)
    for copy in lifted:
        copy.wait_recv()
    advance(mains[3], 4)
    advance(extras, 0)
    for pair in mains:
        advance(pair, 5)

    to_sibling = mail.post(
        tokens.at[:, :, :, :, share_of(half, 1 - core)], sibling.at[...], other
    )

    def score(k, _):
        span = pl.ds(pl.multiple_of(k * 256, 256), 256)
        rows = tokens[...].reshape(group, width)
        value = jnp.dot(rows, embedding_t[:, span], preferred_element_type=F32)
        scores[span, :] = value.T
        return _

    advance(extras, 1)
    lax.fori_loop(0, vocab_local // 256, score, 0)

    def cap(w, carry):
        total, target = carry
        rows = pl.ds(pl.multiple_of(w * 32, 32), 32)
        capped = softcap * jnp.tanh(scores[rows] / softcap)
        allowed, onehot = masks(words[pl.ds(w, 1)], targets[...], vocab_start + w * 32)
        weight = jnp.where(allowed, jnp.exp(capped), 0.0)
        total += weight.reshape(4, 8, group).sum(axis=0)
        target += jnp.where(onehot, capped, 0.0).reshape(4, 8, group).sum(axis=0)
        slope = 1.0 - jnp.square(capped / softcap)
        slopes[rows] = weight * slope
        picks[rows] = jnp.where(onehot, slope, 0.0)
        return total, target

    zero = jnp.zeros((8, group), F32)
    total, target = lax.fori_loop(0, vocab_local // 32, cap, (zero, zero))
    total = total.sum(axis=0, keepdims=True)
    target = target.sum(axis=0, keepdims=True)

    def swap(sums, me, peers):
        sums[me, 0:1] = total
        sums[me, 1:2] = target
        return [mail.post(sums.at[me], sums.at[me], device) for device in peers]

    def summed(sums, copies):
        for copy in copies:
            copy.wait_recv()
        both = sums[...].sum(axis=0)
        return both[0:1], both[1:2]

    def turn(k):
        rows = pl.ds(k * 128, 128)
        slopes_t[:, rows] = slopes[rows].T
        picks_t[:, rows] = picks[rows].T

    copies = swap(plane_sums, y * N + x, [{Y: fold(y + i), X: fold(x + j)} for i, j in plane_peers])
    for k in range(vocab_local // 128):
        turn(k)
    advance(extras, 2)
    total, target = summed(plane_sums, copies)
    copies = swap(depth_sums, z, [{Z: fold(z + d)} for d in range(1, N)])
    advance(extras, 3)
    total, target = summed(depth_sums, copies)
    log_total = jnp.log(total)
    loss[...] = log_total - target
    inverse = 1.0 / total
    inverse_t = jnp.broadcast_to(inverse, (128, group)).T

    for k in range(vocab_local // 128):
        columns = pl.ds(k * 128, 128)
        by_token[:, columns] = (slopes_t[:, columns] * inverse_t - picks_t[:, columns]).astype(BF16)

    def by_vocabulary(k, _):
        rows = pl.ds(pl.multiple_of(k * 32, 32), 32)
        dlogits[0, rows] = (slopes[rows] * inverse - picks[rows]).astype(BF16)
        return _

    def product(k):
        value = jnp.dot(
            by_token[...], embedding[:, pl.ds(k * lane, lane)], preferred_element_type=F32
        )
        part[k] = value.reshape(N, N, N, ROWS, lane)

    def reducer(k, first, second):
        boxes = [b.at[k] for b in (send1, recv1, mid, send2, recv2, last, send3, recv3)]
        return Reduce(mail, part.at[k], boxes, at, first, second, hidden_grad, pl.ds(k * lane, lane))

    lanes = [(k, k + LANES) for k in range(LANES)]
    pairs = [(reducer(i, X, Y), reducer(j, Y, X)) for i, j in lanes]

    def open1(k):
        for i, r in zip(lanes[k], pairs[k]):
            product(i)
            r.open1()

    def run(k, *names):
        for name in names:
            for r in pairs[k]:
                getattr(r, name)()

    def grad(k, source, begin):
        value = jnp.dot(dlogits[k], source.reshape(group, share), preferred_element_type=F32)
        if begin:
            embed_grad[...] = value
        else:
            embed_grad[...] += value

    open1(0)
    lax.fori_loop(0, vocab_local // 32, by_vocabulary, 0)
    around = mail.post(dlogits.at[0], dlogits.at[2], partner)
    beside = mail.post(dlogits.at[0], dlogits.at[1], other)
    open1(1)
    advance(extras, 4)
    run(0, "relay1")
    open1(2)
    run(1, "relay1")
    grad(0, tokens[:, :, :, :, share_of(half, core)], True)
    run(0, "open2")
    run(2, "relay1")
    beside.wait_recv()
    to_sibling.wait_recv()
    grad(1, sibling[...], False)
    run(1, "open2")
    run(0, "relay2")
    run(2, "open2")
    run(1, "relay2")
    run(0, "open3")
    around.wait_recv()
    passed = mail.post(dlogits.at[2], dlogits.at[3], other)
    run(2, "relay2")
    run(1, "open3")
    run(2, "open3")
    advance(extras, 5)
    grad(2, extra[0], False)
    passed.wait_recv()
    grad(3, extra[1], False)
    for k in range(LANES):
        run(k, "finish")
    mail.close()


def write_out(loss, hidden_grad, embed_grad, loss_out, hidden_out, embed_out, sem):
    pairs = ((hidden_grad, hidden_out), (embed_grad, embed_out))
    copies = [pltpu.make_async_copy(a, b, sem.at[k]) for k, (a, b) in enumerate(pairs)]
    for copy in copies:
        copy.start()
    loss_out[...] = loss[0]
    for copy in copies:
        copy.wait()


def on_device(hidden, embedding, targets, grammar_bits):
    rows, width = hidden.shape
    vocab_local = embedding.shape[0]
    group = targets.shape[0]
    share, lane, lanes = width // 4, width // (2 * LANES), 2 * LANES
    vmem = pl.BlockSpec(memory_space=pltpu.VMEM)
    blocks = (N, N, N, ROWS)
    hbm = pl.BlockSpec(memory_space=pltpu.HBM)
    results = pl.pallas_call(
        kernel,
        out_shape=(
            jax.ShapeDtypeStruct((1, group), F32),
            jax.ShapeDtypeStruct((rows, width), F32),
            jax.ShapeDtypeStruct((vocab_local, share), F32),
        ),
        in_specs=[vmem, vmem, vmem, hbm],
        out_specs=(vmem, vmem, vmem),
        scratch_shapes=[
            pltpu.VMEM(blocks + (width,), BF16),
            pltpu.VMEM((2,) + blocks + (share,), BF16),
            pltpu.VMEM(blocks + (share,), BF16),
            pltpu.VMEM((vocab_local, width), BF16),
            pltpu.VMEM((width, vocab_local), BF16),
            pltpu.VMEM((vocab_local, group), F32),
            pltpu.VMEM((vocab_local, group), F32),
            pltpu.VMEM((vocab_local, group), F32),
            pltpu.VMEM((group, vocab_local), F32),
            pltpu.VMEM((group, vocab_local), F32),
            pltpu.VMEM((4, vocab_local, group), BF16),
            pltpu.VMEM((group, vocab_local), BF16),
            pltpu.VMEM((lanes,) + blocks + (lane,), F32),
            pltpu.VMEM((N * N, 2, group), F32),
            pltpu.VMEM((N, 2, group), F32),
            pltpu.VMEM((lanes, 6, N, 2, ROWS, lane), BF16),
            pltpu.VMEM((lanes, 6, N, 2, ROWS, lane), BF16),
            pltpu.VMEM((lanes, N, N, ROWS, lane), F32),
            pltpu.VMEM((lanes, 6, 2, ROWS, lane), F32),
            pltpu.VMEM((lanes, 6, 2, ROWS, lane), F32),
            pltpu.VMEM((lanes, N, ROWS, lane), F32),
            pltpu.VMEM((lanes, N - 1, ROWS, lane), BF16),
            pltpu.VMEM((lanes, N - 1, ROWS, lane), BF16),
            pltpu.SemaphoreType.DMA,
            pltpu.SemaphoreType.DMA((340,)),
            pltpu.SemaphoreType.DMA((340,)),
        ],
        compiler_params=pltpu.CompilerParams(
            collective_id=0, has_side_effects=True, vmem_limit_bytes=50 * 1024 * 1024
        ),
        name="fused",
    )(hidden, grammar_bits.T, targets[None, :], embedding)
    return pl.pallas_call(
        write_out,
        out_shape=(
            jax.ShapeDtypeStruct((group,), F32),
            jax.ShapeDtypeStruct((rows, width), F32),
            jax.ShapeDtypeStruct((vocab_local, share), F32),
        ),
        in_specs=[vmem, vmem, vmem],
        out_specs=(vmem, hbm, hbm),
        scratch_shapes=[pltpu.SemaphoreType.DMA((2,))],
        compiler_params=pltpu.CompilerParams(vmem_limit_bytes=8 * 1024 * 1024),
        name="write_out",
    )(*results)


def solution(mesh):
    split = Mesh(mesh.devices.reshape(2, 2, 4, 4, 4), AXES)
    return jax.shard_map(
        on_device,
        mesh=split,
        in_specs=(P(AXES, None), P(VOCAB, None), P(DP), P(DP, VOCAB)),
        out_specs=(P(DP), P(AXES, None), P(VOCAB, DP)),
        check_vma=False,
    )
```

```python
import functools

import jax
import jax.numpy as jnp
from jax import lax
from jax.experimental import pallas as pl
from jax.experimental.pallas import tpu as pltpu
from jax.sharding import Mesh
from jax.sharding import PartitionSpec as P

AXES = ("dp_0", "dp_1", "vocab_0", "vocab_1", "vocab_2")
VOCAB = ("vocab_0", "vocab_1", "vocab_2")
DP = ("dp_0", "dp_1")
HALF, CORE, Y, Z, X = AXES
MESH = pl.DeviceIdType.MESH
N = 4
ROWS = 8
LANES = 3
softcap = 30.0
F32, BF16 = jnp.float32, jnp.bfloat16


def fold(k):
    return lax.rem(k, N)


def masks(words, targets, first_id):
    rows = 32 * words.shape[0]
    bit = lax.broadcasted_iota(jnp.int32, (32, words.shape[1]), 0)
    spread = [jnp.right_shift(words[k : k + 1], bit) & 1 for k in range(words.shape[0])]
    unpacked = spread[0] if len(spread) == 1 else jnp.concatenate(spread, axis=0)
    ids = first_id + lax.broadcasted_iota(jnp.int32, (rows, words.shape[1]), 0)
    onehot = ids == targets
    return (unpacked == 1) | onehot, onehot


class Mail:
    def __init__(self, send_sem, recv_sem):
        self.send_sem, self.recv_sem = send_sem, recv_sem
        self.count = 0
        self.sent = []

    def describe(self, src, dst, device, send, recv):
        return pltpu.make_async_remote_copy(
            src_ref=src,
            dst_ref=dst,
            send_sem=self.send_sem.at[send],
            recv_sem=self.recv_sem.at[recv],
            device_id=device,
            device_id_type=MESH,
        )

    def start(self, copy):
        copy.start()
        self.sent.append(copy)
        return copy

    def post(self, src, dst, device):
        k = self.count
        self.count += 1
        return self.start(self.describe(src, dst, device, k, k))

    def post_each(self, src, dst, axis, me, steps):
        base = self.count - 1
        self.count += N - 1
        for d in steps:
            self.start(self.describe(src, dst, {axis: fold(me + d)}, base + d, base + N - d))
        return [self.describe(src, dst, {axis: fold(me + d)}, base + d, base + d) for d in steps]

    def close(self, spare=0):
        done = len(self.sent) - spare
        for copy in self.sent[:done]:
            copy.wait_send()
        self.sent = self.sent[done:]


class Gather:
    def __init__(self, mail, view, at, first, second, span):
        self.mail, self.view, self.span = mail, view, span
        self.first, self.second = first, second
        self.u, self.v = at[first], at[second]
        self.relays = []
        self.planes = {}

    def ref(self, u, v, piece):
        y, x = (u, v) if self.first == Y else (v, u)
        return self.view(y, x, self.span[piece])

    def both(self, axis, ref, src=None):
        k = self.u if axis == self.first else self.v
        return [
            self.mail.post(ref if src is None else src, ref, {axis: fold(k + d)}) for d in (1, N - 1)
        ]

    def along_first(self, src=None):
        self.near = self.both(self.first, self.ref(self.u, self.v, 0), src)

    def plane(self, d, src=None):
        self.planes[d] = self.both(self.second, self.ref(fold(self.u + d), self.v, 0), src)

    def relay_first(self):
        before, after = fold(self.u + N - 1), fold(self.u + 1)
        self.near[0].wait_recv()
        low = self.ref(before, self.v, 1)
        self.far = [self.mail.post(low, low, {self.first: after})]
        self.near[1].wait_recv()
        high = self.ref(after, self.v, 2)
        self.far.append(self.mail.post(high, high, {self.first: before}))

    def far_first(self):
        for copy in self.far:
            copy.wait_recv()

    def relay_second(self, d):
        before, after = fold(self.v + N - 1), fold(self.v + 1)
        p = fold(self.u + d)
        self.planes[d][0].wait_recv()
        low = self.ref(p, before, 1)
        self.relays.append(self.mail.post(low, low, {self.second: after}))
        self.planes[d][1].wait_recv()
        high = self.ref(p, after, 2)
        self.relays.append(self.mail.post(high, high, {self.second: before}))

    def finish(self):
        for copy in self.relays:
            copy.wait_recv()


def advance(gathers, step, sources=None):
    if step == 0:
        for k, g in enumerate(gathers):
            g.along_first(sources and sources[k])
        for k, g in enumerate(gathers):
            g.plane(0, sources and sources[k])
    elif step == 1:
        for g in gathers:
            g.relay_first()
            g.plane(N - 1)
            g.plane(1)
    elif step == 2:
        for g in gathers:
            g.relay_second(0)
        for g in gathers:
            g.far_first()
            g.plane(2)
    elif step == 3:
        for g in gathers:
            g.relay_second(N - 1)
            g.relay_second(1)
    elif step == 4:
        for g in gathers:
            g.relay_second(2)
    else:
        for g in gathers:
            g.finish()


class Reduce:
    def __init__(self, mail, part, boxes, at, first, second, out, columns):
        self.mail, self.part, self.at = mail, part, at
        self.send1, self.recv1, self.mid, self.send2, self.recv2, self.last, self.send3, self.recv3 = boxes
        self.first, self.second = first, second
        self.u, self.w = at[first], at[second]
        self.out, self.columns = out, columns

    def partial(self, u, w, start):
        y, x = (w, u) if self.first == X else (u, w)
        return self.part[y, pl.ds(start, 2), x]

    def post1(self, k, d):
        return self.mail.post(self.send1.at[k], self.recv1.at[k], {self.first: fold(self.u + d)})

    def post2(self, k, d):
        return self.mail.post(self.send2.at[k], self.recv2.at[k], {self.second: fold(self.w + d)})

    def open1(self):
        self.one = []
        plan = ((2, 0, 1), (2, 2, N - 1), (1, 2, 1), (N - 1, 0, N - 1))
        for k, (to, start, d) in enumerate(plan):
            u = fold(self.u + to)

            def stage(w, _):
                self.send1[k, w] = self.partial(u, w, start).astype(BF16)
                return _

            lax.fori_loop(0, N, stage, 0)
            self.one.append(self.post1(k, d))

    def relay1(self):
        for k, to, start in ((0, 1, 0), (1, N - 1, 2)):
            self.one[k].wait_recv()
            u = fold(self.u + to)

            def stage(w, _):
                total = self.partial(u, w, start) + self.recv1[k, w].astype(F32)
                self.send1[4 + k, w] = total.astype(BF16)
                return _

            lax.fori_loop(0, N, stage, 0)
            self.one.append(self.post1(4 + k, to))

    def open2(self):
        for k in (2, 3, 4, 5):
            self.one[k].wait_recv()

        def total(w, _):
            self.mid[w, 0:2] = (
                self.partial(self.u, w, 0) + self.recv1[3, w].astype(F32) + self.recv1[4, w].astype(F32)
            )
            self.mid[w, 2:4] = (
                self.partial(self.u, w, 2) + self.recv1[2, w].astype(F32) + self.recv1[5, w].astype(F32)
            )
            return _

        lax.fori_loop(0, N, total, 0)
        self.two = []
        plan = ((2, 0, 1), (2, 2, N - 1), (1, 2, 1), (N - 1, 0, N - 1))
        for k, (to, start, d) in enumerate(plan):
            self.send2[k] = self.mid[fold(self.w + to), start : start + 2].astype(self.send2.dtype)
            self.two.append(self.post2(k, d))

    def relay2(self):
        for k, to, start in ((0, 1, 0), (1, N - 1, 2)):
            self.two[k].wait_recv()
            total = self.mid[fold(self.w + to), start : start + 2] + self.recv2[k].astype(F32)
            self.send2[4 + k] = total.astype(self.send2.dtype)
            self.two.append(self.post2(4 + k, to))

    def open3(self):
        for k in (2, 3, 4, 5):
            self.two[k].wait_recv()
        self.last[0:2] = self.mid[self.w, 0:2] + self.recv2[3].astype(F32) + self.recv2[4].astype(F32)
        self.last[2:4] = self.mid[self.w, 2:4] + self.recv2[2].astype(F32) + self.recv2[5].astype(F32)
        self.three = []
        for d in (2, 1, N - 1):
            z = fold(self.at[Z] + d)
            self.send3[d - 1] = self.last[z].astype(BF16)
            self.three.append(self.mail.post(self.send3.at[d - 1], self.recv3.at[d - 1], {Z: z}))

    def finish(self):
        total = self.last[self.at[Z]]
        for copy in self.three:
            copy.wait_recv()
        for d in range(1, N):
            total += self.recv3[d - 1].astype(F32)
        self.out[:, self.columns] = total


def kernel(
    hidden, words, targets, embedding_hbm,
    loss, hidden_grad, embed_grad,
    tokens, extra, sibling, embedding, embedding_t, scores, slopes, picks, slopes_t, picks_t, dlogits, by_token, part, plane_sums, depth_sums,
    send1, recv1, mid, send2, recv2, last, send3, recv3,
    load_sem, send_sem, recv_sem,
):
    at = {a: lax.axis_index(a) for a in AXES}
    half, core, y, z, x = (at[a] for a in AXES)
    width = hidden.shape[1]
    vocab_local = embedding.shape[0]
    group = tokens.shape[0] * tokens.shape[1] * tokens.shape[2] * ROWS
    color, share, lane = width // 2, width // 4, width // (2 * LANES)
    partner = {HALF: 1 - half}
    across = {HALF: 1 - half, CORE: 1 - core}
    other = {CORE: 1 - core}
    vocab_start = ((y * N + z) * N + x) * vocab_local

    load = pltpu.make_async_copy(embedding_hbm, embedding, load_sem)
    load.start()
    barrier = pltpu.get_barrier_semaphore()
    plane_peers = [(i, j) for i in range(N) for j in range(N) if i or j]
    greeted = [{Y: fold(y + i), X: fold(x + j)} for i, j in plane_peers]
    greeted += [{Z: fold(z + d)} for d in range(1, N)] + [partner, across, other]
    for device in greeted:
        pl.semaphore_signal(barrier, inc=1, device_id=device, device_id_type=MESH)
    pl.semaphore_wait(barrier, len(greeted))

    mail = Mail(send_sem, recv_sem)
    inner = z * (N - 1 - z) // 2
    nearest, middle = 1 + 2 * (z // 2), 2 + inner * (3 - 2 * z)
    order = (nearest, middle, 6 - nearest - middle)
    own = mail.post_each(hidden, tokens.at[y, z, x], Z, z, order)

    def share_of(h, c):
        return pl.ds(pl.multiple_of((2 * h + c) * share, 128), share)

    def slot(k, start, size):
        half_size = size // 2
        zs = pl.ds(k, 1)
        return (
            (zs, pl.ds(start, size)),
            (zs, pl.ds(start, half_size)),
            (zs, pl.ds(start + half_size, half_size)),
        )

    def main_view(yy, xx, piece):
        return tokens.at[yy, piece[0], xx, :, piece[1]]

    def extra_view(k):
        return lambda yy, xx, piece: extra.at[k, yy, piece[0], xx]

    def main_pair(k):
        return [
            Gather(mail, main_view, at, Y, X, slot(k, 0, color)),
            Gather(mail, main_view, at, X, Y, slot(k, color, color)),
        ]

    tokens[y, z, x] = hidden[...]
    mains = [main_pair(z)] + [main_pair(fold(z + d)) for d in order]
    def flip(part):
        blocks = width // 256

        def piece(k, _):
            span = pl.ds(pl.multiple_of((part * blocks + k) * 128, 128), 128)
            embedding_t[span, :] = embedding[:, span].T
            return _

        lax.fori_loop(0, blocks, piece, 0)

    advance(mains[0], 0)
    crossed = [
        mail.post(hidden.at[:, share_of(1 - half, core)], extra.at[0, y, z, x], partner),
        mail.post(hidden.at[:, share_of(1 - half, 1 - core)], extra.at[1, y, z, x], across),
    ]
    depth = ((pl.ds(0, N),), (pl.ds(0, 2),), (pl.ds(2, 2),))
    extras = [
        Gather(mail, extra_view(0), at, Y, X, depth),
        Gather(mail, extra_view(1), at, X, Y, depth),
    ]
    advance(mains[0], 1)
    own[0].wait_recv()
    advance(mains[1], 0)
    advance(mains[0], 2)
    advance(mains[1], 1)
    load.wait()
    flip(0)
    own[1].wait_recv()
    advance(mains[2], 0)
    advance(mains[0], 3)
    own[2].wait_recv()
    advance(mains[3], 0)
    advance(mains[1], 2)
    for copy in crossed:
        copy.wait_recv()
    lifted = mail.post_each(extra.at[:, y, z, x], extra.at[:, y, z, x], Z, z, order)
    advance(mains[2], 1)
    advance(mains[0], 4)
    advance(mains[3], 1)
    advance(mains[1], 3)
    flip(1)
    advance(mains[2], 2)
    advance(mains[1], 4)
    advance(mains[3], 2)
    advance(mains[2], 3)
    advance(mains[3], 3)
    advance(mains[2], 4)
    for copy in lifted:
        copy.wait_recv()
    advance(mains[3], 4)
    advance(extras, 0)
    for pair in mains:
        advance(pair, 5)

    to_sibling = mail.post(
        tokens.at[:, :, :, :, share_of(half, 1 - core)], sibling.at[...], other
    )

    def score(k, _):
        span = pl.ds(pl.multiple_of(k * 256, 256), 256)
        rows = tokens[...].reshape(group, width)
        value = jnp.dot(rows, embedding_t[:, span], preferred_element_type=F32)
        scores[span, :] = value.T
        return _

    advance(extras, 1)
    lax.fori_loop(0, vocab_local // 256, score, 0)

    def cap(w, carry):
        total, target = carry
        rows = pl.ds(pl.multiple_of(w * 32, 32), 32)
        capped = softcap * jnp.tanh(scores[rows] / softcap)
        allowed, onehot = masks(words[pl.ds(w, 1)], targets[...], vocab_start + w * 32)
        weight = jnp.where(allowed, jnp.exp(capped), 0.0)
        total += weight.reshape(4, 8, group).sum(axis=0)
        target += jnp.where(onehot, capped, 0.0).reshape(4, 8, group).sum(axis=0)
        slope = 1.0 - jnp.square(capped / softcap)
        slopes[rows] = weight * slope
        picks[rows] = jnp.where(onehot, slope, 0.0)
        return total, target

    zero = jnp.zeros((8, group), F32)
    total, target = lax.fori_loop(0, vocab_local // 32, cap, (zero, zero))
    total = total.sum(axis=0, keepdims=True)
    target = target.sum(axis=0, keepdims=True)

    def swap(sums, me, peers):
        sums[me, 0:1] = total
        sums[me, 1:2] = target
        return [mail.post(sums.at[me], sums.at[me], device) for device in peers]

    def summed(sums, copies):
        for copy in copies:
            copy.wait_recv()
        both = sums[...].sum(axis=0)
        return both[0:1], both[1:2]

    def turn(k):
        rows = pl.ds(k * 128, 128)
        slopes_t[:, rows] = slopes[rows].T
        picks_t[:, rows] = picks[rows].T

    copies = swap(plane_sums, y * N + x, [{Y: fold(y + i), X: fold(x + j)} for i, j in plane_peers])
    for k in range(vocab_local // 128):
        turn(k)
    advance(extras, 2)
    total, target = summed(plane_sums, copies)
    copies = swap(depth_sums, z, [{Z: fold(z + d)} for d in range(1, N)])
    advance(extras, 3)
    total, target = summed(depth_sums, copies)
    log_total = jnp.log(total)
    loss[...] = log_total - target
    inverse = 1.0 / total
    inverse_t = jnp.broadcast_to(inverse, (128, group)).T

    for k in range(vocab_local // 128):
        columns = pl.ds(k * 128, 128)
        by_token[:, columns] = (slopes_t[:, columns] * inverse_t - picks_t[:, columns]).astype(BF16)

    def by_vocabulary(k, _):
        rows = pl.ds(pl.multiple_of(k * 32, 32), 32)
        dlogits[0, rows] = (slopes[rows] * inverse - picks[rows]).astype(BF16)
        return _

    def product(k):
        value = jnp.dot(
            by_token[...], embedding[:, pl.ds(k * lane, lane)], preferred_element_type=F32
        )
        part[k] = value.reshape(N, N, N, ROWS, lane)

    def reducer(k, first, second):
        boxes = [b.at[k] for b in (send1, recv1, mid, send2, recv2, last, send3, recv3)]
        return Reduce(mail, part.at[k], boxes, at, first, second, hidden_grad, pl.ds(k * lane, lane))

    lanes = [(k, k + LANES) for k in range(LANES)]
    pairs = [(reducer(i, X, Y), reducer(j, Y, X)) for i, j in lanes]

    def open1(k):
        for i, r in zip(lanes[k], pairs[k]):
            product(i)
            r.open1()

    def run(k, *names):
        for name in names:
            for r in pairs[k]:
                getattr(r, name)()

    def grad(k, source, begin):
        value = jnp.dot(dlogits[k], source.reshape(group, share), preferred_element_type=F32)
        if begin:
            embed_grad[...] = value
        else:
            embed_grad[...] += value

    open1(0)
    lax.fori_loop(0, vocab_local // 32, by_vocabulary, 0)
    around = mail.post(dlogits.at[0], dlogits.at[2], partner)
    beside = mail.post(dlogits.at[0], dlogits.at[1], other)
    open1(1)
    advance(extras, 4)
    run(0, "relay1")
    open1(2)
    run(1, "relay1")
    grad(0, tokens[:, :, :, :, share_of(half, core)], True)
    run(0, "open2")
    run(2, "relay1")
    beside.wait_recv()
    to_sibling.wait_recv()
    grad(1, sibling[...], False)
    run(1, "open2")
    run(0, "relay2")
    run(2, "open2")
    run(1, "relay2")
    run(0, "open3")
    around.wait_recv()
    passed = mail.post(dlogits.at[2], dlogits.at[3], other)
    advance(extras, 5)
    grad(2, extra[0], False)
    run(2, "relay2")
    run(1, "open3")
    passed.wait_recv()
    grad(3, extra[1], False)
    run(2, "open3")
    run(0, "finish")
    run(1, "finish")
    mail.close(2 * 2 * (N - 1))
    run(2, "finish")
    mail.close()


def write_out(loss, hidden_grad, embed_grad, loss_out, hidden_out, embed_out, sem):
    pairs = ((hidden_grad, hidden_out), (embed_grad, embed_out))
    copies = [pltpu.make_async_copy(a, b, sem.at[k]) for k, (a, b) in enumerate(pairs)]
    for copy in copies:
        copy.start()
    loss_out[...] = loss[0]
    for copy in copies:
        copy.wait()


def on_device(hidden, embedding, targets, grammar_bits):
    rows, width = hidden.shape
    vocab_local = embedding.shape[0]
    group = targets.shape[0]
    share, lane, lanes = width // 4, width // (2 * LANES), 2 * LANES
    vmem = pl.BlockSpec(memory_space=pltpu.VMEM)
    blocks = (N, N, N, ROWS)
    hbm = pl.BlockSpec(memory_space=pltpu.HBM)
    results = pl.pallas_call(
        kernel,
        out_shape=(
            jax.ShapeDtypeStruct((1, group), F32),
            jax.ShapeDtypeStruct((rows, width), F32),
            jax.ShapeDtypeStruct((vocab_local, share), F32),
        ),
        in_specs=[vmem, vmem, vmem, hbm],
        out_specs=(vmem, vmem, vmem),
        scratch_shapes=[
            pltpu.VMEM(blocks + (width,), BF16),
            pltpu.VMEM((2,) + blocks + (share,), BF16),
            pltpu.VMEM(blocks + (share,), BF16),
            pltpu.VMEM((vocab_local, width), BF16),
            pltpu.VMEM((width, vocab_local), BF16),
            pltpu.VMEM((vocab_local, group), F32),
            pltpu.VMEM((vocab_local, group), F32),
            pltpu.VMEM((vocab_local, group), F32),
            pltpu.VMEM((group, vocab_local), F32),
            pltpu.VMEM((group, vocab_local), F32),
            pltpu.VMEM((4, vocab_local, group), BF16),
            pltpu.VMEM((group, vocab_local), BF16),
            pltpu.VMEM((lanes,) + blocks + (lane,), F32),
            pltpu.VMEM((N * N, 2, group), F32),
            pltpu.VMEM((N, 2, group), F32),
            pltpu.VMEM((lanes, 6, N, 2, ROWS, lane), BF16),
            pltpu.VMEM((lanes, 6, N, 2, ROWS, lane), BF16),
            pltpu.VMEM((lanes, N, N, ROWS, lane), F32),
            pltpu.VMEM((lanes, 6, 2, ROWS, lane), F32),
            pltpu.VMEM((lanes, 6, 2, ROWS, lane), F32),
            pltpu.VMEM((lanes, N, ROWS, lane), F32),
            pltpu.VMEM((lanes, N - 1, ROWS, lane), BF16),
            pltpu.VMEM((lanes, N - 1, ROWS, lane), BF16),
            pltpu.SemaphoreType.DMA,
            pltpu.SemaphoreType.DMA((340,)),
            pltpu.SemaphoreType.DMA((340,)),
        ],
        compiler_params=pltpu.CompilerParams(
            collective_id=0, has_side_effects=True, vmem_limit_bytes=50 * 1024 * 1024
        ),
        name="fused",
    )(hidden, grammar_bits.T, targets[None, :], embedding)
    return pl.pallas_call(
        write_out,
        out_shape=(
            jax.ShapeDtypeStruct((group,), F32),
            jax.ShapeDtypeStruct((rows, width), F32),
            jax.ShapeDtypeStruct((vocab_local, share), F32),
        ),
        in_specs=[vmem, vmem, vmem],
        out_specs=(vmem, hbm, hbm),
        scratch_shapes=[pltpu.SemaphoreType.DMA((2,))],
        compiler_params=pltpu.CompilerParams(vmem_limit_bytes=8 * 1024 * 1024),
        name="write_out",
    )(*results)


def solution(mesh):
    split = Mesh(mesh.devices.reshape(2, 2, 4, 4, 4), AXES)
    return jax.shard_map(
        on_device,
        mesh=split,
        in_specs=(P(AXES, None), P(VOCAB, None), P(DP), P(DP, VOCAB)),
        out_specs=(P(DP), P(AXES, None), P(VOCAB, DP)),
        check_vma=False,
    )
```
